32 devices in a mesh: data: 2 (over x), dap2: 4 (over z), dap: 4 (over y, core).
Axes of the slice: x: 2, y: 2, z: 4, core: 2. Of those that a mesh axis runs over, the one named last changes fastest.
Arguments:
- pair_rep: bfloat16 [512, 256, 128], P(('data', 'dap2', 'dap')), parts along dimension 0
- pair_mask: int32 [512, 256], P(('data', 'dap2', 'dap')), parts along dimension 0
- norm_in: bfloat16 [16, 2, 2, 128], replicated
- norm_out: bfloat16 [16, 2, 2, 128], replicated
- w_ab: bfloat16 [16, 2, 128, 512], replicated
- w_gate: bfloat16 [16, 2, 128, 128], replicated
- w_out: bfloat16 [16, 2, 128, 128], replicated
Outputs:
- output: bfloat16 [512, 256, 128], P(('data', 'dap2', 'dap')), parts along dimension 0
There are 2 independent parts. The reference program is written for one: setup_inputs(seed, part) draws one part's arguments, and reference() takes and returns one part's arrays. A program takes and returns all parts, laid end to end along the dimension named above; an argument that names none is the same for every part.
All inputs are finite; a program needn't handle non-finite values.
Results may differ from the reference program's by a relative error of at most 0.02.
Values are sent between devices in bfloat16 or wider.
A program may use at most 1 GiB of HBM per device.

```python
import jax
import jax.numpy as jnp
from jax import lax

N_RES = 256
C_PAIR = 128
C_HID = 128
N_LAYERS = 16
LN_EPS = 1e-5


def setup_inputs(seed: int = 0, part: int = 0) -> dict:
    base_key = jax.random.key(seed)
    part_key = jax.random.fold_in(base_key, part)
    pair_key, mask_key = jax.random.split(part_key)
    weight_keys = jax.random.split(jax.random.key(seed + 17), 5)
    pair_rep = jax.random.normal(pair_key, (N_RES, N_RES, C_PAIR), jnp.float32).astype(jnp.bfloat16)
    keep_res = (jax.random.randint(mask_key, (N_RES,), 0, 16) != 0).astype(jnp.int32)
    pair_mask = keep_res[:, None] * keep_res[None, :]
    norm_base = jnp.array([1.0, 0.0], jnp.float32)[:, None]
    norm_in = (norm_base + 0.3 * jax.random.normal(weight_keys[0], (N_LAYERS, 2, 2, C_PAIR), jnp.float32)).astype(jnp.bfloat16)
    norm_out = (norm_base + 0.3 * jax.random.normal(weight_keys[1], (N_LAYERS, 2, 2, C_HID), jnp.float32)).astype(jnp.bfloat16)
    w_ab = (jax.random.normal(weight_keys[2], (N_LAYERS, 2, C_PAIR, 4 * C_HID), jnp.float32) * C_PAIR ** -0.5).astype(jnp.bfloat16)
    w_gate = (jax.random.normal(weight_keys[3], (N_LAYERS, 2, C_PAIR, C_PAIR), jnp.float32) * C_PAIR ** -0.5).astype(jnp.bfloat16)
    w_out = (jax.random.normal(weight_keys[4], (N_LAYERS, 2, C_HID, C_PAIR), jnp.float32) * (0.5 * C_HID ** -0.5)).astype(jnp.bfloat16)
    return {"pair_rep": pair_rep, "pair_mask": pair_mask, "norm_in": norm_in, "norm_out": norm_out, "w_ab": w_ab, "w_gate": w_gate, "w_out": w_out}


def layer_norm(values, gain_vec, shift_vec, norm_axis):
    mean_val = jnp.mean(values, axis=norm_axis, keepdims=True)
    centered = values - mean_val
    var_val = jnp.mean(centered * centered, axis=norm_axis, keepdims=True)
    return centered * lax.rsqrt(var_val + LN_EPS) * gain_vec + shift_vec


def tri_update(pair_cur, mask_f, norm_in, norm_out, w_ab, w_gate, w_out, outgoing):
    gain_in = norm_in[0].astype(jnp.float32)
    shift_in = norm_in[1].astype(jnp.float32)
    gain_out = norm_out[0].astype(jnp.float32)
    shift_out = norm_out[1].astype(jnp.float32)

    def row_inputs(row_args):
        x_row = layer_norm(row_args[0].astype(jnp.float32), gain_in, shift_in, -1).astype(jnp.bfloat16)
        proj_row = jnp.dot(x_row, w_ab, preferred_element_type=jnp.float32).reshape(N_RES, 4, C_HID)
        a_row = (row_args[1] * jax.nn.sigmoid(proj_row[:, 1]) * proj_row[:, 0]).astype(jnp.bfloat16)
        b_row = (row_args[1] * jax.nn.sigmoid(proj_row[:, 3]) * proj_row[:, 2]).astype(jnp.bfloat16)
        return a_row, b_row

    def out_channel(ab_pair):
        return jnp.dot(ab_pair[0], ab_pair[1].T, preferred_element_type=jnp.float32).astype(jnp.bfloat16)

    def in_channel(ab_pair):
        return jnp.dot(ab_pair[0].T, ab_pair[1], preferred_element_type=jnp.float32).astype(jnp.bfloat16)

    def row_output(row_args):
        pair_f = row_args[0].astype(jnp.float32)
        x_row = layer_norm(pair_f, gain_in, shift_in, -1).astype(jnp.bfloat16)
        y_row = layer_norm(row_args[1].astype(jnp.float32), gain_out, shift_out, -1).astype(jnp.bfloat16)
        update_val = jnp.dot(y_row, w_out, preferred_element_type=jnp.float32)
        gate_val = jax.nn.sigmoid(jnp.dot(x_row, w_gate, preferred_element_type=jnp.float32))
        return (pair_f + gate_val * update_val).astype(jnp.bfloat16)

    a_val, b_val = lax.map(row_inputs, (pair_cur, mask_f))
    channel_fn = out_channel if outgoing else in_channel
    tri_out = lax.map(channel_fn, (jnp.transpose(a_val, (2, 0, 1)), jnp.transpose(b_val, (2, 0, 1))))
    return lax.map(row_output, (pair_cur, jnp.transpose(tri_out, (1, 2, 0))))


def reference(pair_rep, pair_mask, norm_in, norm_out, w_ab, w_gate, w_out):
    mask_f = pair_mask.astype(jnp.float32)[:, :, None]

    def layer_step(pair_cur, params):
        pair_cur = tri_update(pair_cur, mask_f, params[0][0], params[1][0], params[2][0], params[3][0], params[4][0], True)
        pair_cur = tri_update(pair_cur, mask_f, params[0][1], params[1][1], params[2][1], params[3][1], params[4][1], False)
        return pair_cur, None

    return lax.scan(layer_step, pair_rep, (norm_in, norm_out, w_ab, w_gate, w_out))[0]
```

```python
import functools

import jax
import jax.numpy as jnp
from jax import lax
from jax.experimental import pallas as pl
from jax.experimental.pallas import tpu as pltpu
from jax.sharding import PartitionSpec as P

LN_EPS = 1e-5
ALL_ROWS = ("data", "dap2", "dap")
MESH = pl.DeviceIdType.MESH
F32, BF16 = jnp.float32, jnp.bfloat16
C = 128
CO = C // 2
LANES = 128
Y_PITCH = 132


def layer_norm(v, gain, shift):
    centered = v - jnp.sum(v, axis=0, keepdims=True) * (1.0 / C)
    var = jnp.sum(centered * centered, axis=0, keepdims=True) * (1.0 / C)
    return (centered * lax.rsqrt(var + LN_EPS) * gain + shift).astype(BF16)


def dot(lhs, rhs, dims=((1,), (0,))):
    return lax.dot_general(lhs, rhs, (dims, ((), ())), preferred_element_type=F32)


def kernel(nz, ny, n_upd, z_in, m_in, w_in, n_in, out, z_ref, x_ref, ab_ref, t_ref, ts_ref, abs_ref, s_ref, y_ref,
           m_ref, w_ref, n_ref, in_sem, w_sem, zsend, zrecv, msend, mrecv, ab_send, ab_recv, t_send, t_recv):
    G = z_in.shape[0]
    NR = z_ref.shape[0]
    NG = NR // G
    N = 2 * NR
    ST = s_ref.shape[1] // (2 * C)
    zi = lax.axis_index("dap2")
    dap = lax.axis_index("dap")
    yi, side = dap // 2, dap % 2
    q = zi * ny + yi
    partner = {"dap": yi * 2 + 1 - side}
    ypeer = {"dap": (1 - yi) * 2 + side}
    up, down = {"dap2": zi + 1}, {"dap2": zi - 1}
    mine = pl.multiple_of(side * NR, NR)

    barrier = pltpu.get_barrier_semaphore()
    pl.semaphore_signal(barrier, inc=1, device_id=partner, device_id_type=MESH)
    if ny > 1:
        pl.semaphore_signal(barrier, inc=1, device_id=ypeer, device_id_type=MESH)

    @pl.when(zi < nz - 1)
    def _():
        pl.semaphore_signal(barrier, inc=1, device_id=up, device_id_type=MESH)

    @pl.when(zi > 0)
    def _():
        pl.semaphore_signal(barrier, inc=1, device_id=down, device_id_type=MESH)

    def params(s):
        slot = s % 2
        return (
            pltpu.make_async_copy(w_in.at[s], w_ref.at[slot], w_sem.at[slot, 0]),
            pltpu.make_async_copy(n_in.at[s], n_ref.at[slot], w_sem.at[slot, 1]),
        )

    for s in range(2):
        for cp in params(s):
            cp.start()

    def rows_of(block):
        return pl.ds(pl.multiple_of(block * G, G), G)

    loads = (
        pltpu.make_async_copy(z_in, z_ref.at[rows_of(q)], in_sem.at[0]),
        pltpu.make_async_copy(m_in, m_ref.at[:, rows_of(q)], in_sem.at[1]),
    )
    for cp in loads:
        cp.start()
    for cp in loads:
        cp.wait()

    neighbours = (2 if ny > 1 else 1) + jnp.where(zi < nz - 1, 1, 0) + jnp.where(zi > 0, 1, 0)
    pl.semaphore_wait(barrier, neighbours)

    def block_copies(block, to, k):
        rows = rows_of(block)
        return (
            pltpu.make_async_remote_copy(z_ref.at[rows], z_ref.at[rows], zsend.at[k], zrecv.at[k], device_id=to, device_id_type=MESH),
            pltpu.make_async_remote_copy(m_ref.at[:, rows], m_ref.at[:, rows], msend.at[k], mrecv.at[k], device_id=to, device_id_type=MESH),
        )

    K_DOWN, K_Y = nz - 1, 2 * (nz - 1)

    def start(copies):
        for cp in copies:
            cp.start()

    def gather(step):
        d = step
        if d == 0:
            if ny > 1:
                start(block_copies(q, ypeer, K_Y + zi))
        have_low, have_high = zi - d >= 0, zi + d <= nz - 1
        low, high = (zi - d) * ny + yi, (zi + d) * ny + yi
        if d > 0:
            @pl.when(have_low)
            def _():
                for cp in block_copies(low, up, d - 1):
                    cp.wait_recv()
                if ny > 1:
                    start(block_copies(low, ypeer, K_Y + zi - d))

            @pl.when(have_high)
            def _():
                for cp in block_copies(high, down, K_DOWN + d - 1):
                    cp.wait_recv()
                if ny > 1:
                    start(block_copies(high, ypeer, K_Y + zi + d))
        if d < nz - 1:
            @pl.when(jnp.logical_and(have_low, zi < nz - 1))
            def _():
                start(block_copies(low, up, d))

            @pl.when(jnp.logical_and(have_high, zi > 0))
            def _():
                start(block_copies(high, down, K_DOWN + d))

    for d in range(nz):
        gather(d)
    if ny > 1:
        for zz in range(nz):
            for cp in block_copies(zz * ny + 1 - yi, ypeer, K_Y + zz):
                cp.wait_recv()
    for d in range(nz - 1):
        @pl.when(jnp.logical_and(zi - d >= 0, zi < nz - 1))
        def _():
            for cp in block_copies((zi - d) * ny + yi, up, d):
                cp.wait_send()

        @pl.when(jnp.logical_and(zi + d <= nz - 1, zi > 0))
        def _():
            for cp in block_copies((zi + d) * ny + yi, down, K_DOWN + d):
                cp.wait_send()
    if ny > 1:
        for zz in range(nz):
            for cp in block_copies(zz * ny + yi, ypeer, K_Y + zz):
                cp.wait_send()

    def swap_t(g):
        @pl.loop(0, C, step=16)
        def _(c0):
            for dc in range(16):
                for h in range(2):
                    v = t_ref[c0 + dc, h, rows_of(g), :].astype(F32)
                    y_ref[h, pl.ds(c0 + dc, G, stride=Y_PITCH), :] = v

    def finish_row(g, r, slot):
        row = g * G + r
        y = [layer_norm(y_ref[h, pl.ds(r * Y_PITCH, C), :], n_ref[slot, 2], n_ref[slot, 3]) for h in range(2)]
        upd = dot(w_ref[slot, 5 * C:6 * C, :], jnp.concatenate(y, axis=1))
        gate = dot(w_ref[slot, 4 * C:5 * C, :], jnp.concatenate([x_ref[row, 0], x_ref[row, 1]], axis=1))
        z_new = []
        for h in range(2):
            ls = slice(h * LANES, (h + 1) * LANES)
            zn = (z_ref[row, h].astype(F32) + (jnp.tanh(gate[:, ls]) + 1.0) * upd[:, ls]).astype(BF16)
            z_ref[row, h] = zn
            z_new.append(zn)
        return z_new

    def start_row(g, r, slot, z_row):
        row = g * G + r
        xm = []
        for h in range(2):
            x = layer_norm(z_row[h].astype(F32), n_ref[slot, 0], n_ref[slot, 1])
            x_ref[row, h] = x
            mask = jnp.broadcast_to(m_ref[h, pl.ds(row, 1), :], (16, LANES)).astype(BF16)
            xm.append(x * jnp.concatenate([mask] * (C // 16), axis=0))
        p = dot(w_ref[slot, 0:4 * C, :], jnp.concatenate(xm, axis=1))
        for ab in range(2):
            for h in range(2):
                ls = slice(h * LANES, (h + 1) * LANES)
                val, gate = p[2 * ab * C:(2 * ab + 1) * C, ls], p[(2 * ab + 1) * C:(2 * ab + 2) * C, ls]
                s_ref[h, pl.ds(ab * C * ST + r, C, stride=ST), :] = val * (jnp.tanh(gate) + 1.0)

    def ab_copy(g):
        slot = g % 2
        return pltpu.make_async_remote_copy(
            abs_ref.at[slot], ab_ref.at[:, :, :, pl.ds(pl.multiple_of(mine + g * G, G), G), :],
            ab_send.at[slot], ab_recv.at[g], device_id=partner, device_id_type=MESH)

    def spread_ab(g):
        @pl.when(g >= 2)
        def _():
            ab_copy(g - 2).wait_send()

        own, other = side * CO, (1 - side) * CO
        rows = pl.ds(pl.multiple_of(mine + g * G, G), G)

        @pl.loop(0, CO, step=8)
        def _(c0):
            for dc in range(8):
                for ab in range(2):
                    for h in range(2):
                        c = c0 + dc
                        ab_ref[ab, c, h, rows, :] = s_ref[h, pl.ds((ab * C + own + c) * ST, G), :].astype(BF16)
                        abs_ref[g % 2, ab, c, h] = s_ref[h, pl.ds((ab * C + other + c) * ST, G), :].astype(BF16)

        ab_copy(g).start()

    def drain_ab():
        for g in range(NG - 2, NG):
            ab_copy(g).wait_send()

    TB = 8

    def t_copy(cb):
        return pltpu.make_async_remote_copy(
            ts_ref.at[pl.ds(cb * TB, TB)], t_ref.at[pl.ds(side * CO + cb * TB, TB)],
            t_send.at[cb], t_recv.at[cb], device_id=partner, device_id_type=MESH)

    def triangle(outgoing):
        @pl.loop(0, CO // TB)
        def _(cb):
            for dc in range(TB):
                c = cb * TB + dc
                b = jnp.concatenate([ab_ref[1, c, 0], ab_ref[1, c, 1]], axis=1)
                if outgoing:
                    theirs = pl.multiple_of(NR - mine, NR)
                    a = jnp.concatenate([jnp.concatenate([ab_ref[0, c, h, pl.ds(r0, NR), :] for h in range(2)], axis=1)
                                         for r0 in (mine, theirs)], axis=0)
                    t = dot(a, b, ((1,), (1,)))
                else:
                    a = jnp.concatenate([ab_ref[0, c, side], ab_ref[0, c, 1 - side]], axis=1)
                    t = dot(a, b, ((0,), (0,)))
                t = t.astype(BF16)
                for h in range(2):
                    ls = slice(h * LANES, (h + 1) * LANES)
                    t_ref[side * CO + c, h] = t[:NR, ls]
                    ts_ref[c, h] = t[NR:, ls]
            t_copy(cb).start()

    def recv_ab():
        for g in range(NG):
            ab_copy(g).wait_recv()

    def recv_t():
        for cb in range(CO // TB):
            t_copy(cb).wait_recv()

    def drain_t():
        for cb in range(CO // TB):
            t_copy(cb).wait_send()

    for cp in params(0):
        cp.wait()

    @pl.loop(0, NG)
    def _(g):
        @pl.loop(0, G, step=2)
        def _(r):
            for dr in range(2):
                row = g * G + r + dr
                start_row(g, r + dr, 0, [z_ref[row, 0], z_ref[row, 1]])
        spread_ab(g)
    drain_ab()

    @pl.loop(0, n_upd)
    def _(u):
        recv_ab()

        @pl.when(u % 2 == 0)
        def _():
            triangle(True)

        @pl.when(u % 2 == 1)
        def _():
            triangle(False)

        @pl.when(u < n_upd - 1)
        def _():
            for cp in params(u + 2):
                cp.start()

        slot = (u + 1) % 2
        for cp in params(u + 1):
            cp.wait()
        recv_t()

        @pl.when(u < n_upd - 1)
        def _():
            @pl.loop(0, NG)
            def _(g):
                swap_t(g)

                @pl.loop(0, G, step=2)
                def _(r):
                    for dr in range(2):
                        start_row(g, r + dr, slot, finish_row(g, r + dr, slot))
                spread_ab(g)
            drain_ab()
        drain_t()

    slot = n_upd % 2
    swap_t(q)

    @pl.loop(0, G, step=2)
    def _(r):
        for dr in range(2):
            finish_row(q, r + dr, slot)
    cp = pltpu.make_async_copy(z_ref.at[rows_of(q)], out, in_sem.at[0])
    cp.start()
    cp.wait()


def pack_params(norm_in, norm_out, w_ab, w_gate, w_out):
    n_upd = w_ab.shape[0] * 2

    def flat(w):
        return w.reshape((n_upd,) + w.shape[2:])

    wab, wg, wo = (jnp.swapaxes(flat(w) * jnp.asarray(0.5, BF16), 1, 2) for w in (w_ab, w_gate, w_out))
    w = jnp.zeros((n_upd + 1, 6 * C, C), BF16)
    w = w.at[:n_upd, :4 * C].set(wab).at[1:, 4 * C:5 * C].set(wg).at[1:, 5 * C:].set(wo)
    n = jnp.zeros((n_upd + 1, 4, C), F32)
    n = n.at[:n_upd, :2].set(flat(norm_in).astype(F32)).at[1:, 2:].set(flat(norm_out).astype(F32))
    return w, jnp.broadcast_to(n[..., None], n.shape + (LANES,))


def solution(mesh):
    nz, ny = mesh.shape["dap2"], mesh.shape["dap"] // 2
    row_spec = P(ALL_ROWS, None, None)
    mask_spec = P(ALL_ROWS, None)

    def local_stack(pair_rep, pair_mask, norm_in, norm_out, w_ab, w_gate, w_out):
        G, N = pair_rep.shape[:2]
        NR, n_upd = N // 2, 2 * w_ab.shape[0]
        chips = nz * ny
        w, n = pack_params(norm_in, norm_out, w_ab, w_gate, w_out)
        z = jnp.transpose(pair_rep.reshape(G, chips, 2, G, C), (0, 2, 4, 1, 3)).reshape(G, 2, C, NR)
        m = jnp.transpose(pair_mask.astype(F32).reshape(G, chips, 2, G), (2, 0, 1, 3)).reshape(2, G, NR)
        ST = G + 1
        anyspec = pl.BlockSpec(memory_space=pl.ANY)
        dma = pltpu.SemaphoreType.DMA
        n_gather = 2 * (nz - 1) + nz
        o = pl.pallas_call(
            functools.partial(kernel, nz, ny, n_upd),
            out_shape=jax.ShapeDtypeStruct(z.shape, BF16),
            in_specs=[anyspec] * 4,
            out_specs=anyspec,
            scratch_shapes=[
                pltpu.VMEM((NR, 2, C, LANES), BF16),
                pltpu.VMEM((NR, 2, C, LANES), BF16),
                pltpu.VMEM((2, CO, 2, N, LANES), BF16),
                pltpu.VMEM((C, 2, NR, LANES), BF16),
                pltpu.VMEM((CO, 2, NR, LANES), BF16),
                pltpu.VMEM((2, 2, CO, 2, G, LANES), BF16),
                pltpu.VMEM((2, 2 * C * ST, LANES), F32),
                pltpu.VMEM((2, G * Y_PITCH, LANES), F32),
                pltpu.VMEM((2, NR, LANES), F32),
                pltpu.VMEM((2, 6 * C, C), BF16),
                pltpu.VMEM((2, 4, C, LANES), F32),
                dma((2,)), dma((2, 2)),
                dma((n_gather,)), dma((n_gather,)), dma((n_gather,)), dma((n_gather,)),
                dma((2,)), dma((NR // G,)), dma((8,)), dma((8,)),
            ],
            compiler_params=pltpu.CompilerParams(collective_id=0, has_side_effects=True, vmem_limit_bytes=67043328),
        )(z, m, w, n)
        o = o.reshape(G, 2, C, chips, G)
        return jnp.transpose(o, (0, 3, 1, 4, 2)).reshape(G, N, C)

    return jax.shard_map(local_stack, mesh=mesh, in_specs=(row_spec, mask_spec, P(), P(), P(), P(), P()), out_specs=row_spec, check_vma=False)
```

```python
import functools

import jax
import jax.numpy as jnp
from jax import lax
from jax.experimental import pallas as pl
from jax.experimental.pallas import tpu as pltpu
from jax.sharding import PartitionSpec as P

LN_EPS = 1e-5
ALL_ROWS = ("data", "dap2", "dap")
MESH = pl.DeviceIdType.MESH
F32, BF16 = jnp.float32, jnp.bfloat16
C = 128
CO = C // 2
LANES = 128
Y_PITCH = 132
R = 4
TB = 8


def total(v):
    parts = [v[32 * k:32 * k + 32] for k in range(4)]
    s = (parts[0] + parts[1]) + (parts[2] + parts[3])
    return jnp.sum(s, axis=0, keepdims=True)


def layer_norm(v, gain, shift):
    centered = v - total(v) * (1.0 / C)
    var = total(centered * centered) * (1.0 / C)
    return (centered * lax.rsqrt(var + LN_EPS) * gain + shift).astype(BF16)


def dot(lhs, rhs, dims=((1,), (0,))):
    return lax.dot_general(lhs, rhs, (dims, ((), ())), preferred_element_type=F32)


def half(h):
    return slice(h * LANES, (h + 1) * LANES)


def kernel(nz, ny, n_upd, z_in, m_in, norms, wab_in, wg_in, wo_in, out, z_ref, x_ref, ab_ref, t_ref, ts_ref, abs_ref,
           s_ref, y_ref, yb_ref, m_ref, mi_ref, wr_ref, w_ref, n_ref, in_sem, w_sem, zsend, zrecv, msend, mrecv,
           ab_send, ab_recv, t_send, t_recv):
    G = z_in.shape[0]
    NR = 2 * G * nz * ny // 2
    NG = NR // G
    ST = G + 1
    NB = NR // R
    BG = G // R
    chips = nz * ny
    zi = lax.axis_index("dap2")
    dap = lax.axis_index("dap")
    yi, side = dap // 2, dap % 2
    q = zi * ny + yi
    partner = {"dap": yi * 2 + 1 - side}
    ypeer = {"dap": (1 - yi) * 2 + side}
    up, down = {"dap2": zi + 1}, {"dap2": zi - 1}
    mine = pl.multiple_of(side * NR, NR)
    theirs = pl.multiple_of(NR - side * NR, NR)

    barrier = pltpu.get_barrier_semaphore()
    pl.semaphore_signal(barrier, inc=1, device_id=partner, device_id_type=MESH)
    if ny > 1:
        pl.semaphore_signal(barrier, inc=1, device_id=ypeer, device_id_type=MESH)

    @pl.when(zi < nz - 1)
    def _():
        pl.semaphore_signal(barrier, inc=1, device_id=up, device_id_type=MESH)

    @pl.when(zi > 0)
    def _():
        pl.semaphore_signal(barrier, inc=1, device_id=down, device_id_type=MESH)

    def rows_of(block):
        return pl.ds(pl.multiple_of(block * G, G), G)

    def weight_copies(s):
        now, before = jnp.minimum(s, n_upd - 1), jnp.clip(s - 1, 0, n_upd - 1)
        return (
            pltpu.make_async_copy(wab_in.at[now], wr_ref.at[:, pl.ds(0, 4 * C)], w_sem.at[0]),
            pltpu.make_async_copy(wg_in.at[before], wr_ref.at[:, pl.ds(4 * C, C)], w_sem.at[1]),
            pltpu.make_async_copy(wo_in.at[before], wr_ref.at[:, pl.ds(5 * C, C)], w_sem.at[2]),
        )

    def start(copies):
        for cp in copies:
            cp.start()

    def prepare(s):
        for cp in weight_copies(s):
            cp.wait()
        for k in range(6):
            w_ref[k * C:(k + 1) * C, :] = (wr_ref[:, k * C:(k + 1) * C] * jnp.asarray(0.5, BF16)).T
        now, before = jnp.minimum(s, n_upd - 1), jnp.clip(s - 1, 0, n_upd - 1)
        for k in range(2):
            n_ref[k] = jnp.broadcast_to(norms[pl.ds(now * 2 + k, 1), :], (C, C)).T
            n_ref[2 + k] = jnp.broadcast_to(norms[pl.ds((n_upd + before) * 2 + k, 1), :], (C, C)).T

    start(weight_copies(0))

    loads = (
        pltpu.make_async_copy(z_in, ts_ref.at[pl.ds(0, G)], in_sem.at[0]),
        pltpu.make_async_copy(m_in, mi_ref, in_sem.at[1]),
    )
    start(loads)
    for cp in loads:
        cp.wait()
    at = lax.broadcasted_iota(jnp.int32, (2 * NR, 2 * NR), 0)
    to = lax.broadcasted_iota(jnp.int32, (2 * NR, 2 * NR), 1)
    source = (to % NR) // G * (2 * G) + to // NR * G + to % G
    order = jnp.where(at == source, 1.0, 0.0).astype(BF16)
    m_perm = dot(mi_ref[...].astype(F32).astype(BF16), order)
    for h in range(2):
        m_ref[h, rows_of(q), :] = m_perm[:, half(h)]

    def pieces(h):
        return [divmod((k * 2 + h) * G, LANES) for k in range(chips)]

    @pl.loop(0, G)
    def _(r):
        for h in range(2):
            rows = [ts_ref[r, a, b:b + G, :] for a, b in pieces(h)]
            z_ref[q * G + r, h] = jnp.concatenate(rows, axis=0).T

    neighbours = (2 if ny > 1 else 1) + jnp.where(zi < nz - 1, 1, 0) + jnp.where(zi > 0, 1, 0)
    pl.semaphore_wait(barrier, neighbours)

    def block_copies(block, to, k):
        rows = rows_of(block)
        return (
            pltpu.make_async_remote_copy(z_ref.at[rows], z_ref.at[rows], zsend.at[k], zrecv.at[k], device_id=to, device_id_type=MESH),
            pltpu.make_async_remote_copy(m_ref.at[:, rows], m_ref.at[:, rows], msend.at[k], mrecv.at[k], device_id=to, device_id_type=MESH),
        )

    K_DOWN, K_Y = nz - 1, 2 * (nz - 1)

    def gather(d):
        if d == 0 and ny > 1:
            start(block_copies(q, ypeer, K_Y + zi))
        have_low, have_high = zi - d >= 0, zi + d <= nz - 1
        low, high = (zi - d) * ny + yi, (zi + d) * ny + yi
        if d > 0:
            @pl.when(have_low)
            def _():
                for cp in block_copies(low, up, d - 1):
                    cp.wait_recv()
                if ny > 1:
                    start(block_copies(low, ypeer, K_Y + zi - d))

            @pl.when(have_high)
            def _():
                for cp in block_copies(high, down, K_DOWN + d - 1):
                    cp.wait_recv()
                if ny > 1:
                    start(block_copies(high, ypeer, K_Y + zi + d))
        if d < nz - 1:
            @pl.when(jnp.logical_and(have_low, zi < nz - 1))
            def _():
                start(block_copies(low, up, d))

            @pl.when(jnp.logical_and(have_high, zi > 0))
            def _():
                start(block_copies(high, down, K_DOWN + d))

    for d in range(nz):
        gather(d)
    prepare(0)
    start(weight_copies(1))
    if ny > 1:
        for zz in range(nz):
            for cp in block_copies(zz * ny + 1 - yi, ypeer, K_Y + zz):
                cp.wait_recv()
    for d in range(nz - 1):
        @pl.when(jnp.logical_and(zi - d >= 0, zi < nz - 1))
        def _():
            for cp in block_copies((zi - d) * ny + yi, up, d):
                cp.wait_send()

        @pl.when(jnp.logical_and(zi + d <= nz - 1, zi > 0))
        def _():
            for cp in block_copies((zi + d) * ny + yi, down, K_DOWN + d):
                cp.wait_send()
    if ny > 1:
        for zz in range(nz):
            for cp in block_copies(zz * ny + yi, ypeer, K_Y + zz):
                cp.wait_send()

    def swap_t(g, c0, n, slot):
        t, y = t_ref.at[pl.ds(c0, n), :, rows_of(g), :], y_ref.at[slot]
        for dc in range(n):
            for h in range(2):
                y[h, pl.ds(c0 + dc, G, stride=Y_PITCH), :] = t[dc, h].astype(F32)

    def out_norm(r, slot):
        return [layer_norm(y_ref[slot, h, pl.ds(r * Y_PITCH, C), :], n_ref[2], n_ref[3]) for h in range(2)]

    def out_dots(row, y):
        upd = dot(w_ref[5 * C:6 * C, :], jnp.concatenate(y, axis=1))
        gate = dot(w_ref[4 * C:5 * C, :], jnp.concatenate([x_ref[row, 0], x_ref[row, 1]], axis=1))
        return upd, gate

    def new_z(row, upd, gate):
        z_row = [(z_ref[row, h].astype(F32) + (jnp.tanh(gate[:, half(h)]) + 1.0) * upd[:, half(h)]).astype(BF16) for h in range(2)]
        for h in range(2):
            z_ref[row, h] = z_row[h]
        return z_row

    def in_norm(row, z_row):
        for h in range(2):
            x_ref[row, h] = layer_norm(z_row[h].astype(F32), n_ref[0], n_ref[1])

    def ab_dot(row):
        x = []
        for h in range(2):
            mask = jnp.broadcast_to(m_ref[h, pl.ds(row, 1), :], (16, LANES)).astype(BF16)
            x.append(x_ref[row, h] * jnp.concatenate([mask] * (C // 16), axis=0))
        return dot(w_ref[0:4 * C, :], jnp.concatenate(x, axis=1))

    def ab_store(p, r, slot):
        for ab in range(2):
            for h in range(2):
                val, gate = p[2 * ab * C:(2 * ab + 1) * C, half(h)], p[(2 * ab + 1) * C:(2 * ab + 2) * C, half(h)]
                s_ref[slot, h, pl.ds(ab * C * ST + r, C, stride=ST), :] = val * (jnp.tanh(gate) + 1.0)

    CB = CO // BG
    LBG = BG.bit_length() - 1

    def ab_copy(k):
        c0 = pl.multiple_of((k & (BG - 1)) * CB, CB)
        rows = pl.ds(pl.multiple_of(mine + (k >> LBG) * G, G), G)
        return pltpu.make_async_remote_copy(
            abs_ref.at[(k & (BG - 1))], ab_ref.at[:, pl.ds(c0, CB), :, rows, :],
            ab_send.at[(k & (BG - 1))], ab_recv.at[(k & (BG - 1))], device_id=partner, device_id_type=MESH)

    def spread_ab(k):
        g, c0 = (k >> LBG), (k & (BG - 1)) * CB
        own, other = (side * CO + c0) * ST, ((1 - side) * CO + c0) * ST
        s = s_ref.at[(g & 1)]
        here = ab_ref.at[:, pl.ds(c0, CB), :, pl.ds(pl.multiple_of(mine + g * G, G), G), :]
        there = abs_ref.at[(k & (BG - 1))]
        for dc in range(CB):
            for ab in range(2):
                for h in range(2):
                    here[ab, dc, h] = s[h, pl.ds(own + (ab * C + dc) * ST, G), :].astype(BF16)
                    there[ab, dc, h] = s[h, pl.ds(other + (ab * C + dc) * ST, G), :].astype(BF16)

    def send_ab(k):
        @pl.when(k >= 0)
        def _():
            ab_copy(k).start()

        @pl.when(k + 1 >= BG)
        def _():
            ab_copy(k + 1 - BG).wait_send()

    def finish_ab():
        @pl.loop(NB - BG, NB)
        def _(k):
            spread_ab(k)
            send_ab(k)
        for k in range(NB - BG + 1, NB):
            ab_copy(k).wait_send()

    def t_copy(cb):
        n = CO // TB
        return pltpu.make_async_remote_copy(
            ts_ref.at[pl.ds(cb * n, n)], t_ref.at[pl.ds(side * CO + cb * n, n)],
            t_send.at[cb], t_recv.at[cb], device_id=partner, device_id_type=MESH)

    def triangle(outgoing, c):
        b = jnp.concatenate([ab_ref[1, c, 0], ab_ref[1, c, 1]], axis=1)
        if outgoing:
            a = jnp.concatenate([jnp.concatenate([ab_ref[0, c, h, pl.ds(r0, NR), :] for h in range(2)], axis=1)
                                 for r0 in (mine, theirs)], axis=0)
            t = dot(a, b, ((1,), (1,)))
        else:
            a = jnp.concatenate([ab_ref[0, c, side], ab_ref[0, c, 1 - side]], axis=1)
            t = dot(a, b, ((0,), (0,)))
        t = t.astype(BF16)
        for h in range(2):
            t_ref[side * CO + c, h] = t[:NR, half(h)]
            ts_ref[c, h] = t[NR:, half(h)]

    def triangles(outgoing):
        @pl.loop(0, TB)
        def _(cb):
            @pl.when(cb % (TB // BG) == 0 if BG < TB else cb >= 0)
            def _():
                for k in range(max(1, BG // TB)):
                    b = cb * BG // TB + k
                    arrived = ab_ref.at[:, pl.ds(b * CB, CB), :, pl.ds(theirs, NR), :]
                    pltpu.make_async_copy(arrived, arrived, ab_recv.at[b]).wait()
            for dc in range(CO // TB):
                triangle(outgoing, cb * (CO // TB) + dc)
            t_copy(cb).start()

    def step_row(it, behind):
        return jnp.where(it < behind, NR, (it - behind) * R)

    @pl.loop(0, NB + 1)
    def _(it):
        row, k = step_row(it, 1), it - 1 - BG
        dots = [ab_dot(row + i) for i in range(R)]
        spread_ab(jnp.maximum(k, 0))
        for i in range(R):
            in_norm(it * R + i, [z_ref[it * R + i, 0], z_ref[it * R + i, 1]])
        prev = it - 1 + 2 * BG
        for i in range(R):
            ab_store(dots[i], (prev & (BG - 1)) * R + i, ((prev >> LBG) & 1))
        send_ab(k)
    finish_ab()

    @pl.loop(0, n_upd)
    def _(u):
        @pl.when(u % 2 == 0)
        def _():
            triangles(True)

        @pl.when(u % 2 == 1)
        def _():
            triangles(False)

        prepare(u + 1)
        start(weight_copies(u + 2))
        for cb in range(TB):
            t_copy(cb).wait_recv()

        @pl.when(u < n_upd - 1)
        def _():
            for c0 in range(0, C, 16):
                swap_t(0, c0, 16, 0)

            @pl.loop(0, NB + 2)
            def _(it):
                k = it - 2 - BG
                row1, row2 = step_row(it, 1), step_row(it, 2)
                outs = [out_dots(row1 + i, [yb_ref[(it + 1) & 1, i, h] for h in range(2)]) for i in range(R)]
                dots = [ab_dot(row2 + i) for i in range(R)]
                for i in range(R):
                    y = out_norm((it & (BG - 1)) * R + i, (it >> LBG) & 1)
                    for h in range(2):
                        yb_ref[it & 1, i, h] = y[h]
                spread_ab(jnp.maximum(k, 0))
                swap_t(jnp.minimum((it >> LBG) + 1, NG - 1), (it & (BG - 1)) * (C // BG), C // BG, ((it >> LBG) + 1) & 1)
                for i in range(R):
                    in_norm(row1 + i, new_z(row1 + i, *outs[i]))
                prev = it - 2 + 2 * BG
                for i in range(R):
                    ab_store(dots[i], (prev & (BG - 1)) * R + i, (prev >> LBG) & 1)
                send_ab(k)
            finish_ab()
        for cb in range(TB):
            t_copy(cb).wait_send()

    for cp in weight_copies(0):
        cp.wait()
    for c0 in range(0, C, 16):
        swap_t(q, c0, 16, 0)

    @pl.loop(0, G)
    def _(r):
        row = q * G + r
        z_row = new_z(row, *out_dots(row, out_norm(r, 0)))
        for h in range(2):
            z_t = z_row[h].T
            for k, (a, b) in enumerate(pieces(h)):
                ts_ref[r, a, b:b + G, :] = z_t[k * G:(k + 1) * G]
    cp = pltpu.make_async_copy(ts_ref.at[pl.ds(0, G)], out, in_sem.at[0])
    cp.start()
    cp.wait()


def solution(mesh):
    nz, ny = mesh.shape["dap2"], mesh.shape["dap"] // 2
    row_spec = P(ALL_ROWS, None, None)
    mask_spec = P(ALL_ROWS, None)

    def local_stack(pair_rep, pair_mask, norm_in, norm_out, w_ab, w_gate, w_out):
        G, N = pair_rep.shape[:2]
        NR, n_upd = N // 2, 2 * w_ab.shape[0]
        norms = jnp.concatenate([norm_in.reshape(-1, C), norm_out.reshape(-1, C)]).astype(F32)
        BG = G // R
        anyspec = pl.BlockSpec(memory_space=pl.ANY)
        vmem = pl.BlockSpec(memory_space=pltpu.VMEM)
        dma = pltpu.SemaphoreType.DMA
        n_gather = 2 * (nz - 1) + nz
        o = pl.pallas_call(
            functools.partial(kernel, nz, ny, n_upd),
            out_shape=jax.ShapeDtypeStruct((G, 2, NR, C), BF16),
            in_specs=[anyspec, anyspec, vmem, anyspec, anyspec, anyspec],
            out_specs=anyspec,
            scratch_shapes=[
                pltpu.VMEM((NR + R, 2, C, LANES), BF16),
                pltpu.VMEM((NR + R, 2, C, LANES), BF16),
                pltpu.VMEM((2, CO, 2, N, LANES), BF16),
                pltpu.VMEM((C, 2, NR, LANES), BF16),
                pltpu.VMEM((CO, 2, NR, LANES), BF16),
                pltpu.VMEM((BG, 2, CO // BG, 2, G, LANES), BF16),
                pltpu.VMEM((2, 2, 2 * C * (G + 1), LANES), F32),
                pltpu.VMEM((2, 2, G * Y_PITCH, LANES), F32),
                pltpu.VMEM((2, R, 2, C, LANES), BF16),
                pltpu.VMEM((2, NR + R, LANES), F32),
                pltpu.VMEM((G, N), jnp.int32),
                pltpu.VMEM((C, 6 * C), BF16),
                pltpu.VMEM((6 * C, C), BF16),
                pltpu.VMEM((4, C, LANES), F32),
                dma((2,)), dma((3,)),
                dma((n_gather,)), dma((n_gather,)), dma((n_gather,)), dma((n_gather,)),
                dma((BG,)), dma((BG,)), dma((TB,)), dma((TB,)),
            ],
            compiler_params=pltpu.CompilerParams(collective_id=0, has_side_effects=True, vmem_limit_bytes=67043328),
        )(pair_rep.reshape(G, 2, NR, C), pair_mask, norms, w_ab.reshape(n_upd, C, 4 * C), w_gate.reshape(n_upd, C, C), w_out.reshape(n_upd, C, C))
        return o.reshape(G, N, C)

    return jax.shard_map(local_stack, mesh=mesh, in_specs=(row_spec, mask_spec, P(), P(), P(), P(), P()), out_specs=row_spec, check_vma=False)
```

```python
import functools

import jax
import jax.numpy as jnp
from jax import lax
from jax.experimental import pallas as pl
from jax.experimental.pallas import tpu as pltpu
from jax.sharding import PartitionSpec as P

LN_EPS = 1e-5
ALL_ROWS = ("data", "dap2", "dap")
MESH = pl.DeviceIdType.MESH
F32, BF16 = jnp.float32, jnp.bfloat16
C = 128
CO = C // 2
LANES = 128
Y_PITCH = 132
R = 4
TB = 8


def total(v):
    parts = [v[32 * k:32 * k + 32] for k in range(4)]
    s = (parts[0] + parts[1]) + (parts[2] + parts[3])
    return jnp.sum(s, axis=0, keepdims=True)


def layer_norm(v, gain, shift):
    centered = v - total(v) * (1.0 / C)
    var = total(centered * centered) * (1.0 / C)
    return (centered * lax.rsqrt(var + LN_EPS) * gain + shift).astype(BF16)


def dot(lhs, rhs, dims=((1,), (0,))):
    return lax.dot_general(lhs, rhs, (dims, ((), ())), preferred_element_type=F32)


def half(h):
    return slice(h * LANES, (h + 1) * LANES)


def kernel(nz, ny, n_upd, z_in, m_in, norms, wab_in, wg_in, wo_in, out, z_ref, x_ref, ab_ref, t_ref, ts_ref, abs_ref,
           s_ref, y_ref, yb_ref, m_ref, mi_ref, wr_ref, w_ref, n_ref, in_sem, w_sem, zsend, zrecv, msend, mrecv,
           ab_send, ab_recv, t_send, t_recv):
    G = z_in.shape[0]
    NR = 2 * G * nz * ny // 2
    NG = NR // G
    ST = G + 1
    NB = NR // R
    BG = G // R
    chips = nz * ny
    zi = lax.axis_index("dap2")
    dap = lax.axis_index("dap")
    yi, side = dap // 2, dap % 2
    q = zi * ny + yi
    partner = {"dap": yi * 2 + 1 - side}
    ypeer = {"dap": (1 - yi) * 2 + side}
    up, down = {"dap2": zi + 1}, {"dap2": zi - 1}
    mine = pl.multiple_of(side * NR, NR)
    theirs = pl.multiple_of(NR - side * NR, NR)

    barrier = pltpu.get_barrier_semaphore()
    pl.semaphore_signal(barrier, inc=1, device_id=partner, device_id_type=MESH)
    if ny > 1:
        pl.semaphore_signal(barrier, inc=1, device_id=ypeer, device_id_type=MESH)

    @pl.when(zi < nz - 1)
    def _():
        pl.semaphore_signal(barrier, inc=1, device_id=up, device_id_type=MESH)

    @pl.when(zi > 0)
    def _():
        pl.semaphore_signal(barrier, inc=1, device_id=down, device_id_type=MESH)

    def rows_of(block):
        return pl.ds(pl.multiple_of(block * G, G), G)

    def weight_copies(s):
        now, before = jnp.minimum(s, n_upd - 1), jnp.clip(s - 1, 0, n_upd - 1)
        return (
            pltpu.make_async_copy(wab_in.at[now], wr_ref.at[:, pl.ds(0, 4 * C)], w_sem.at[0]),
            pltpu.make_async_copy(wg_in.at[before], wr_ref.at[:, pl.ds(4 * C, C)], w_sem.at[1]),
            pltpu.make_async_copy(wo_in.at[before], wr_ref.at[:, pl.ds(5 * C, C)], w_sem.at[2]),
        )

    def start(copies):
        for cp in copies:
            cp.start()

    def prepare(s):
        for cp in weight_copies(s):
            cp.wait()
        for k in range(6):
            w_ref[k * C:(k + 1) * C, :] = (wr_ref[:, k * C:(k + 1) * C] * jnp.asarray(0.5, BF16)).T
        now, before = jnp.minimum(s, n_upd - 1), jnp.clip(s - 1, 0, n_upd - 1)
        for k in range(2):
            n_ref[k] = jnp.broadcast_to(norms[pl.ds(now * 2 + k, 1), :], (C, C)).T
            n_ref[2 + k] = jnp.broadcast_to(norms[pl.ds((n_upd + before) * 2 + k, 1), :], (C, C)).T

    start(weight_copies(0))

    loads = (
        pltpu.make_async_copy(z_in, ts_ref.at[pl.ds(0, G)], in_sem.at[0]),
        pltpu.make_async_copy(m_in, mi_ref, in_sem.at[1]),
    )
    start(loads)
    for cp in loads:
        cp.wait()
    at = lax.broadcasted_iota(jnp.int32, (2 * NR, 2 * NR), 0)
    to = lax.broadcasted_iota(jnp.int32, (2 * NR, 2 * NR), 1)
    source = (to % NR) // G * (2 * G) + to // NR * G + to % G
    order = jnp.where(at == source, 1.0, 0.0).astype(BF16)
    m_perm = dot(mi_ref[...].astype(F32).astype(BF16), order)
    for h in range(2):
        m_ref[h, rows_of(q), :] = m_perm[:, half(h)]

    def pieces(h):
        return [divmod((k * 2 + h) * G, LANES) for k in range(chips)]

    @pl.loop(0, G, step=4)
    def _(r0):
        for i in range(4):
            for h in range(2):
                rows = [ts_ref[r0 + i, a, b:b + G, :] for a, b in pieces(h)]
                z_ref[q * G + r0 + i, h] = jnp.concatenate(rows, axis=0).T

    neighbours = (2 if ny > 1 else 1) + jnp.where(zi < nz - 1, 1, 0) + jnp.where(zi > 0, 1, 0)
    pl.semaphore_wait(barrier, neighbours)

    def block_copies(block, to, k):
        rows = rows_of(block)
        return (
            pltpu.make_async_remote_copy(z_ref.at[rows], z_ref.at[rows], zsend.at[k], zrecv.at[k], device_id=to, device_id_type=MESH),
            pltpu.make_async_remote_copy(m_ref.at[:, rows], m_ref.at[:, rows], msend.at[k], mrecv.at[k], device_id=to, device_id_type=MESH),
        )

    K_DOWN, K_Y = nz - 1, 2 * (nz - 1)

    def gather(d):
        if d == 0 and ny > 1:
            start(block_copies(q, ypeer, K_Y + zi))
        have_low, have_high = zi - d >= 0, zi + d <= nz - 1
        low, high = (zi - d) * ny + yi, (zi + d) * ny + yi
        if d > 0:
            @pl.when(have_low)
            def _():
                for cp in block_copies(low, up, d - 1):
                    cp.wait_recv()
                if ny > 1:
                    start(block_copies(low, ypeer, K_Y + zi - d))

            @pl.when(have_high)
            def _():
                for cp in block_copies(high, down, K_DOWN + d - 1):
                    cp.wait_recv()
                if ny > 1:
                    start(block_copies(high, ypeer, K_Y + zi + d))
        if d < nz - 1:
            @pl.when(jnp.logical_and(have_low, zi < nz - 1))
            def _():
                start(block_copies(low, up, d))

            @pl.when(jnp.logical_and(have_high, zi > 0))
            def _():
                start(block_copies(high, down, K_DOWN + d))

    def nearest(k):
        order = [sorted(range(nz), key=lambda z: (abs(z - me), z)) for me in range(nz)]
        return sum(jnp.where(zi == me, order[me][k], 0) for me in range(nz))

    arrivals = [(q, [lambda: gather(0)])]
    for k in range(1, nz):
        arrivals.append((nearest(k) * ny + yi, [functools.partial(gather, k)]))
        if ny > 1:
            arrivals.append((nearest(k - 1) * ny + 1 - yi, []))
    if ny > 1:
        arrivals.append((nearest(nz - 1) * ny + 1 - yi, []))

    def await_y(block):
        for cp in block_copies(block, ypeer, K_Y + block // ny):
            cp.wait_recv()

    def arrived(pos):
        block, calls = arrivals[pos]
        for call in calls:
            call()
        if not calls:
            await_y(block)

    def first_group(pos):
        return sum(jnp.where(pos == k, block, 0) for k, (block, _) in enumerate(arrivals))

    def drain_gather():
        for d in range(nz - 1):
            @pl.when(jnp.logical_and(zi - d >= 0, zi < nz - 1))
            def _():
                for cp in block_copies((zi - d) * ny + yi, up, d):
                    cp.wait_send()

            @pl.when(jnp.logical_and(zi + d <= nz - 1, zi > 0))
            def _():
                for cp in block_copies((zi + d) * ny + yi, down, K_DOWN + d):
                    cp.wait_send()
        if ny > 1:
            for zz in range(nz):
                for cp in block_copies(zz * ny + yi, ypeer, K_Y + zz):
                    cp.wait_send()

    arrived(0)
    prepare(0)
    start(weight_copies(1))

    def swap_t(g, c0, n, slot):
        t, y = t_ref.at[pl.ds(c0, n), :, rows_of(g), :], y_ref.at[slot]
        for dc in range(n):
            for h in range(2):
                y[h, pl.ds(c0 + dc, G, stride=Y_PITCH), :] = t[dc, h].astype(F32)

    def out_norm(r, slot):
        return [layer_norm(y_ref[slot, h, pl.ds(r * Y_PITCH, C), :], n_ref[2], n_ref[3]) for h in range(2)]

    def out_dots(row, y):
        upd = dot(w_ref[5 * C:6 * C, :], jnp.concatenate(y, axis=1))
        gate = dot(w_ref[4 * C:5 * C, :], jnp.concatenate([x_ref[row, 0], x_ref[row, 1]], axis=1))
        return upd, gate

    def new_z(row, upd, gate):
        z_row = [(z_ref[row, h].astype(F32) + (jnp.tanh(gate[:, half(h)]) + 1.0) * upd[:, half(h)]).astype(BF16) for h in range(2)]
        for h in range(2):
            z_ref[row, h] = z_row[h]
        return z_row

    def in_norm(row, z_row):
        for h in range(2):
            x_ref[row, h] = layer_norm(z_row[h].astype(F32), n_ref[0], n_ref[1])

    def ab_dot(row):
        x = []
        for h in range(2):
            mask = jnp.broadcast_to(m_ref[h, pl.ds(row, 1), :], (16, LANES)).astype(BF16)
            x.append(x_ref[row, h] * jnp.concatenate([mask] * (C // 16), axis=0))
        return dot(w_ref[0:4 * C, :], jnp.concatenate(x, axis=1))

    def ab_store(p, r, slot):
        for ab in range(2):
            for h in range(2):
                val, gate = p[2 * ab * C:(2 * ab + 1) * C, half(h)], p[(2 * ab + 1) * C:(2 * ab + 2) * C, half(h)]
                s_ref[slot, h, pl.ds(ab * C * ST + r, C, stride=ST), :] = val * (jnp.tanh(gate) + 1.0)

    CB = CO // BG
    LBG = BG.bit_length() - 1

    def same(g):
        return g

    def ab_copy(k, group=same):
        c0 = pl.multiple_of((k & (BG - 1)) * CB, CB)
        rows = pl.ds(pl.multiple_of(mine + group(k >> LBG) * G, G), G)
        return pltpu.make_async_remote_copy(
            abs_ref.at[(k & (BG - 1))], ab_ref.at[:, pl.ds(c0, CB), :, rows, :],
            ab_send.at[(k & (BG - 1))], ab_recv.at[(k & (BG - 1))], device_id=partner, device_id_type=MESH)

    def spread_ab(k, group=same):
        g, c0 = (k >> LBG), (k & (BG - 1)) * CB
        own, other = (side * CO + c0) * ST, ((1 - side) * CO + c0) * ST
        s = s_ref.at[(g & 1)]
        here = ab_ref.at[:, pl.ds(c0, CB), :, pl.ds(pl.multiple_of(mine + group(g) * G, G), G), :]
        there = abs_ref.at[(k & (BG - 1))]
        for dc in range(CB):
            for ab in range(2):
                for h in range(2):
                    here[ab, dc, h] = s[h, pl.ds(own + (ab * C + dc) * ST, G), :].astype(BF16)
                    there[ab, dc, h] = s[h, pl.ds(other + (ab * C + dc) * ST, G), :].astype(BF16)

    def send_ab(k, group=same):
        @pl.when(k >= 0)
        def _():
            ab_copy(k, group).start()

        @pl.when(k + 1 >= BG)
        def _():
            ab_copy(k + 1 - BG, group).wait_send()

    def finish_ab(group=same):
        @pl.loop(NB - BG, NB)
        def _(k):
            spread_ab(k, group)
            send_ab(k, group)

    def drain_ab():
        for k in range(NB - BG + 1, NB):
            ab_copy(k).wait_send()

    EARLY = min(2, NG) * G

    def t_copy(c0, n, row0, rows, k):
        c0, rows = pl.multiple_of(c0, n), pl.ds(row0, rows)
        return pltpu.make_async_remote_copy(
            ts_ref.at[pl.ds(c0, n), :, rows, :], t_ref.at[pl.ds(side * CO + c0, n), :, rows, :],
            t_send.at[k], t_recv.at[k], device_id=partner, device_id_type=MESH)

    def early_t():
        return t_copy(0, CO, 0, EARLY, 0)

    def late_t(g):
        return t_copy(0, CO, pl.multiple_of(g * G, G), G, g)

    def recv_t(g):
        late_t(g).wait_recv()

    def triangle(outgoing, c):
        b = jnp.concatenate([ab_ref[1, c, 0], ab_ref[1, c, 1]], axis=1)
        if outgoing:
            a = jnp.concatenate([jnp.concatenate([ab_ref[0, c, h, pl.ds(r0, NR), :] for h in range(2)], axis=1)
                                 for r0 in (mine, theirs)], axis=0)
            t = dot(a, b, ((1,), (1,)))
        else:
            a = jnp.concatenate([ab_ref[0, c, side], ab_ref[0, c, 1 - side]], axis=1)
            t = dot(a, b, ((0,), (0,)))
        t = t.astype(BF16)
        for h in range(2):
            t_ref[side * CO + c, h] = t[:NR, half(h)]
            ts_ref[c, h] = t[NR:, half(h)]

    def triangles(outgoing):
        @pl.loop(0, TB)
        def _(cb):
            @pl.when(cb % (TB // BG) == 0 if BG < TB else cb >= 0)
            def _():
                for k in range(max(1, BG // TB)):
                    b = cb * BG // TB + k
                    arrived = ab_ref.at[:, pl.ds(b * CB, CB), :, pl.ds(theirs, NR), :]
                    pltpu.make_async_copy(arrived, arrived, ab_recv.at[b]).wait()
            for dc in range(CO // TB):
                triangle(outgoing, cb * (CO // TB) + dc)
            t_copy(cb * (CO // TB), CO // TB, 0, EARLY, 0).start()
        for g in range(EARLY // G, NG):
            late_t(g).start()

    def step_row(it, behind):
        return jnp.where(it < behind, NR, (it - behind) * R)

    @pl.loop(0, NB + 1)
    def _(it):
        for pos in range(1, len(arrivals)):
            @pl.when(it == pos * BG)
            def _(pos=pos):
                arrived(pos)

        def row_of(step):
            return first_group(step >> LBG) * G + (step & (BG - 1)) * R

        k = it - 1 - BG
        row, now = jnp.where(it == 0, NR, row_of(it - 1)), jnp.where(it == NB, NR, row_of(it))
        dots = [ab_dot(row + i) for i in range(R)]
        spread_ab(jnp.maximum(k, 0), first_group)
        for i in range(R):
            in_norm(now + i, [z_ref[now + i, 0], z_ref[now + i, 1]])
        prev = it - 1 + 2 * BG
        for i in range(R):
            ab_store(dots[i], (prev & (BG - 1)) * R + i, (prev >> LBG) & 1)
        send_ab(k, first_group)
    finish_ab(first_group)
    drain_gather()

    @pl.loop(0, n_upd)
    def _(u):
        prepare(u + 1)
        start(weight_copies(u + 2))

        @pl.when(u % 2 == 0)
        def _():
            triangles(True)

        @pl.when(u % 2 == 1)
        def _():
            triangles(False)

        drain_ab()
        early_t().wait_recv()

        @pl.when(u < n_upd - 1)
        def _():
            for c0 in range(0, C, 16):
                swap_t(0, c0, 16, 0)

            @pl.loop(0, NB + 2)
            def _(it):
                k = it - 2 - BG
                row1, row2 = step_row(it, 1), step_row(it, 2)
                outs = [out_dots(row1 + i, [yb_ref[(it + 1) & 1, i, h] for h in range(2)]) for i in range(R)]
                dots = [ab_dot(row2 + i) for i in range(R)]
                for i in range(R):
                    y = out_norm((it & (BG - 1)) * R + i, (it >> LBG) & 1)
                    for h in range(2):
                        yb_ref[it & 1, i, h] = y[h]
                spread_ab(jnp.maximum(k, 0))
                swap_t(jnp.minimum((it >> LBG) + 1, NG - 1), (it & (BG - 1)) * (C // BG), C // BG, ((it >> LBG) + 1) & 1)
                for i in range(R):
                    in_norm(row1 + i, new_z(row1 + i, *outs[i]))
                prev = it - 2 + 2 * BG
                for i in range(R):
                    ab_store(dots[i], (prev & (BG - 1)) * R + i, (prev >> LBG) & 1)
                send_ab(k)

                @pl.when(jnp.logical_and(((it + 1) & (BG - 1)) == 0, it + 1 < NB - BG))
                def _():
                    recv_t(((it + 1) >> LBG) + 1)
            finish_ab()

        @pl.when(u == n_upd - 1)
        def _():
            for g in range(EARLY // G, NG):
                recv_t(g)
        early_t().wait_send()
        for g in range(EARLY // G, NG):
            late_t(g).wait_send()

    for cp in weight_copies(0):
        cp.wait()
    for c0 in range(0, C, 16):
        swap_t(q, c0, 16, 0)

    @pl.loop(0, G, step=4)
    def _(r0):
        outs = [out_dots(q * G + r0 + i, out_norm(r0 + i, 0)) for i in range(4)]
        for i in range(4):
            z_row = new_z(q * G + r0 + i, *outs[i])
            for h in range(2):
                z_t = z_row[h].T
                for k, (a, b) in enumerate(pieces(h)):
                    ts_ref[r0 + i, a, b:b + G, :] = z_t[k * G:(k + 1) * G]
    cp = pltpu.make_async_copy(ts_ref.at[pl.ds(0, G)], out, in_sem.at[0])
    cp.start()
    cp.wait()


def solution(mesh):
    nz, ny = mesh.shape["dap2"], mesh.shape["dap"] // 2
    row_spec = P(ALL_ROWS, None, None)
    mask_spec = P(ALL_ROWS, None)

    def local_stack(pair_rep, pair_mask, norm_in, norm_out, w_ab, w_gate, w_out):
        G, N = pair_rep.shape[:2]
        NR, n_upd = N // 2, 2 * w_ab.shape[0]
        norms = jnp.concatenate([norm_in.reshape(-1, C), norm_out.reshape(-1, C)]).astype(F32)
        BG = G // R
        anyspec = pl.BlockSpec(memory_space=pl.ANY)
        vmem = pl.BlockSpec(memory_space=pltpu.VMEM)
        dma = pltpu.SemaphoreType.DMA
        n_gather = 2 * (nz - 1) + nz
        o = pl.pallas_call(
            functools.partial(kernel, nz, ny, n_upd),
            out_shape=jax.ShapeDtypeStruct((G, 2, NR, C), BF16),
            in_specs=[anyspec, anyspec, vmem, anyspec, anyspec, anyspec],
            out_specs=anyspec,
            scratch_shapes=[
                pltpu.VMEM((NR + R, 2, C, LANES), BF16),
                pltpu.VMEM((NR + R, 2, C, LANES), BF16),
                pltpu.VMEM((2, CO, 2, N, LANES), BF16),
                pltpu.VMEM((C, 2, NR, LANES), BF16),
                pltpu.VMEM((CO, 2, NR, LANES), BF16),
                pltpu.VMEM((BG, 2, CO // BG, 2, G, LANES), BF16),
                pltpu.VMEM((2, 2, 2 * C * (G + 1), LANES), F32),
                pltpu.VMEM((2, 2, G * Y_PITCH, LANES), F32),
                pltpu.VMEM((2, R, 2, C, LANES), BF16),
                pltpu.VMEM((2, NR + R, LANES), F32),
                pltpu.VMEM((G, N), jnp.int32),
                pltpu.VMEM((C, 6 * C), BF16),
                pltpu.VMEM((6 * C, C), BF16),
                pltpu.VMEM((4, C, LANES), F32),
                dma((2,)), dma((3,)),
                dma((n_gather,)), dma((n_gather,)), dma((n_gather,)), dma((n_gather,)),
                dma((BG,)), dma((BG,)), dma((NR // G,)), dma((NR // G,)),
            ],
            compiler_params=pltpu.CompilerParams(collective_id=0, has_side_effects=True, vmem_limit_bytes=67043328),
        )(pair_rep.reshape(G, 2, NR, C), pair_mask, norms, w_ab.reshape(n_upd, C, 4 * C), w_gate.reshape(n_upd, C, C), w_out.reshape(n_upd, C, C))
        return o.reshape(G, N, C)

    return jax.shard_map(local_stack, mesh=mesh, in_specs=(row_spec, mask_spec, P(), P(), P(), P(), P()), out_specs=row_spec, check_vma=False)
```

```python
import functools

import jax
import jax.numpy as jnp
from jax import lax
from jax.experimental import pallas as pl
from jax.experimental.pallas import tpu as pltpu
from jax.sharding import PartitionSpec as P

LN_EPS = 1e-5
ALL_ROWS = ("data", "dap2", "dap")
MESH = pl.DeviceIdType.MESH
F32, BF16 = jnp.float32, jnp.bfloat16
C = 128
CO = C // 2
LANES = 128
Y_PITCH = 129
R = 4
TB = 4
ORDER = (
    ("u", 0), ("g", 0), ("a", 0), ("g", 2), ("u", 2), ("a", 2),
    ("u", 1), ("u", 3), ("g", 1), ("a", 1), ("g", 3), ("a", 3),
)
WB = 16


def total(v):
    parts = [v[32 * k:32 * k + 32] for k in range(4)]
    s = (parts[0] + parts[1]) + (parts[2] + parts[3])
    return jnp.sum(s, axis=0, keepdims=True)


def layer_norm(v, gain, shift):
    centered = v - total(v) * (1.0 / C)
    var = total(centered * centered) * (1.0 / C)
    return (centered * lax.rsqrt(var + LN_EPS) * gain + shift).astype(BF16)


def dot(lhs, rhs, dims=((1,), (0,))):
    return lax.dot_general(lhs, rhs, (dims, ((), ())), preferred_element_type=F32)


def half(h):
    return slice(h * LANES, (h + 1) * LANES)


def kernel(nz, ny, n_upd, z_in, m_in, norms, wab_in, wg_in, wo_in, out, z_ref, x_ref, ab_ref, t_ref, ts_ref, abs_ref,
           s_ref, y_ref, yb_ref, m_ref, mi_ref, wr_ref, w_ref, n_ref, in_sem, w_sem, zsend, zrecv, msend, mrecv,
           ab_send, ab_recv, t_send, t_recv):
    G = z_in.shape[0]
    NR = 2 * G * nz * ny // 2
    NG = NR // G
    ST = G + 1
    NB = NR // R
    BG = G // R
    chips = nz * ny
    zi = lax.axis_index("dap2")
    dap = lax.axis_index("dap")
    yi, side = dap // 2, dap % 2
    q = zi * ny + yi
    partner = {"dap": yi * 2 + 1 - side}
    ypeer = {"dap": (1 - yi) * 2 + side}
    up, down = {"dap2": zi + 1}, {"dap2": zi - 1}
    mine = pl.multiple_of(side * NR, NR)
    theirs = pl.multiple_of(NR - side * NR, NR)

    barrier = pltpu.get_barrier_semaphore()
    pl.semaphore_signal(barrier, inc=1, device_id=partner, device_id_type=MESH)
    if ny > 1:
        pl.semaphore_signal(barrier, inc=1, device_id=ypeer, device_id_type=MESH)

    @pl.when(zi < nz - 1)
    def _():
        pl.semaphore_signal(barrier, inc=1, device_id=up, device_id_type=MESH)

    @pl.when(zi > 0)
    def _():
        pl.semaphore_signal(barrier, inc=1, device_id=down, device_id_type=MESH)

    def rows_of(block):
        return pl.ds(pl.multiple_of(block * G, G), G)

    def weight_copies(s):
        now, before = jnp.minimum(s, n_upd - 1), jnp.clip(s - 1, 0, n_upd - 1)
        return (
            pltpu.make_async_copy(wab_in.at[now], wr_ref.at[:, pl.ds(0, 4 * C)], w_sem.at[0]),
            pltpu.make_async_copy(wg_in.at[before], wr_ref.at[:, pl.ds(4 * C, C)], w_sem.at[1]),
            pltpu.make_async_copy(wo_in.at[before], wr_ref.at[:, pl.ds(5 * C, C)], w_sem.at[2]),
        )

    def start(copies):
        for cp in copies:
            cp.start()

    def prepare(s):
        for cp in weight_copies(s):
            cp.wait()
        for k in range(6):
            w = (wr_ref[:, k * C:(k + 1) * C] * jnp.asarray(0.5, BF16)).T
            if k >= 4:
                w_ref[k * C:(k + 1) * C, :] = w
            else:
                for c in range(0, C, WB):
                    at = k // 2 * 2 * C + 2 * c + k % 2 * WB
                    w_ref[at:at + WB, :] = w[c:c + WB]
        now, before = jnp.minimum(s, n_upd - 1), jnp.clip(s - 1, 0, n_upd - 1)
        for k in range(2):
            n_ref[k] = jnp.broadcast_to(norms[pl.ds(now * 2 + k, 1), :], (C, C)).T
            n_ref[2 + k] = jnp.broadcast_to(norms[pl.ds((n_upd + before) * 2 + k, 1), :], (C, C)).T

    start(weight_copies(0))

    loads = (
        pltpu.make_async_copy(z_in, ts_ref.at[pl.ds(0, G)], in_sem.at[0]),
        pltpu.make_async_copy(m_in, mi_ref, in_sem.at[1]),
    )
    start(loads)
    for cp in loads:
        cp.wait()
    at = lax.broadcasted_iota(jnp.int32, (2 * NR, 2 * NR), 0)
    to = lax.broadcasted_iota(jnp.int32, (2 * NR, 2 * NR), 1)
    source = (to % NR) // G * (2 * G) + to // NR * G + to % G
    order = jnp.where(at == source, 1.0, 0.0).astype(BF16)
    m_perm = dot(mi_ref[...].astype(F32).astype(BF16), order)
    for h in range(2):
        m_ref[h, rows_of(q), :] = m_perm[:, half(h)]

    def pieces(h):
        return [divmod((k * 2 + h) * G, LANES) for k in range(chips)]

    @pl.loop(0, G, step=4)
    def _(r0):
        for i in range(4):
            for h in range(2):
                rows = [ts_ref[r0 + i, a, b:b + G, :] for a, b in pieces(h)]
                z_ref[q * G + r0 + i, h] = jnp.concatenate(rows, axis=0).T

    neighbours = (2 if ny > 1 else 1) + jnp.where(zi < nz - 1, 1, 0) + jnp.where(zi > 0, 1, 0)
    pl.semaphore_wait(barrier, neighbours)

    def block_copies(block, to, k):
        rows = rows_of(block)
        return (
            pltpu.make_async_remote_copy(z_ref.at[rows], z_ref.at[rows], zsend.at[k], zrecv.at[k], device_id=to, device_id_type=MESH),
            pltpu.make_async_remote_copy(m_ref.at[:, rows], m_ref.at[:, rows], msend.at[k], mrecv.at[k], device_id=to, device_id_type=MESH),
        )

    K_DOWN, K_Y = nz - 1, 2 * (nz - 1)

    def gather(d):
        if d == 0 and ny > 1:
            start(block_copies(q, ypeer, K_Y + zi))
        have_low, have_high = zi - d >= 0, zi + d <= nz - 1
        low, high = (zi - d) * ny + yi, (zi + d) * ny + yi
        if d > 0:
            @pl.when(have_low)
            def _():
                for cp in block_copies(low, up, d - 1):
                    cp.wait_recv()
                if ny > 1:
                    start(block_copies(low, ypeer, K_Y + zi - d))

            @pl.when(have_high)
            def _():
                for cp in block_copies(high, down, K_DOWN + d - 1):
                    cp.wait_recv()
                if ny > 1:
                    start(block_copies(high, ypeer, K_Y + zi + d))
        if d < nz - 1:
            @pl.when(jnp.logical_and(have_low, zi < nz - 1))
            def _():
                start(block_copies(low, up, d))

            @pl.when(jnp.logical_and(have_high, zi > 0))
            def _():
                start(block_copies(high, down, K_DOWN + d))

    def nearest(k):
        order = [sorted(range(nz), key=lambda z: (abs(z - me), z)) for me in range(nz)]
        return sum(jnp.where(zi == me, order[me][k], 0) for me in range(nz))

    arrivals = [(q, [lambda: gather(0)])]
    for k in range(1, nz):
        arrivals.append((nearest(k) * ny + yi, [functools.partial(gather, k)]))
        if ny > 1:
            arrivals.append((nearest(k - 1) * ny + 1 - yi, []))
    if ny > 1:
        arrivals.append((nearest(nz - 1) * ny + 1 - yi, []))

    def await_y(block):
        for cp in block_copies(block, ypeer, K_Y + block // ny):
            cp.wait_recv()

    def arrived(pos):
        block, calls = arrivals[pos]
        for call in calls:
            call()
        if not calls:
            await_y(block)

    def first_group(pos):
        return sum(jnp.where(pos == k, block, 0) for k, (block, _) in enumerate(arrivals))

    def drain_gather():
        for d in range(nz - 1):
            @pl.when(jnp.logical_and(zi - d >= 0, zi < nz - 1))
            def _():
                for cp in block_copies((zi - d) * ny + yi, up, d):
                    cp.wait_send()

            @pl.when(jnp.logical_and(zi + d <= nz - 1, zi > 0))
            def _():
                for cp in block_copies((zi + d) * ny + yi, down, K_DOWN + d):
                    cp.wait_send()
        if ny > 1:
            for zz in range(nz):
                for cp in block_copies(zz * ny + yi, ypeer, K_Y + zz):
                    cp.wait_send()

    arrived(0)
    prepare(0)
    start(weight_copies(1))

    def swap_t(g, c0, n, slot):
        t, y = t_ref.at[pl.ds(c0, n), :, rows_of(g), :], y_ref.at[slot]
        for dc in range(n):
            for h in range(2):
                y[h, pl.ds(c0 + dc, G, stride=Y_PITCH), :] = t[dc, h].astype(F32)

    def out_norm(r, slot):
        return [layer_norm(y_ref[slot, h, pl.ds(r * Y_PITCH, C), :], n_ref[2], n_ref[3]) for h in range(2)]

    def upd_dot(y):
        return dot(w_ref[5 * C:6 * C, :], jnp.concatenate(y, axis=1))

    def gate_dot(row):
        return dot(w_ref[4 * C:5 * C, :], jnp.concatenate([x_ref[row, 0], x_ref[row, 1]], axis=1))

    def new_z(row, upd, gate):
        z_row = [(z_ref[row, h].astype(F32) + (jnp.tanh(gate[:, half(h)]) + 1.0) * upd[:, half(h)]).astype(BF16) for h in range(2)]
        for h in range(2):
            z_ref[row, h] = z_row[h]
        return z_row

    def in_norm(row, z_row):
        for h in range(2):
            x_ref[row, h] = layer_norm(z_row[h].astype(F32), n_ref[0], n_ref[1])

    def ab_dot(row):
        x = []
        for h in range(2):
            mask = jnp.broadcast_to(m_ref[h, pl.ds(row, 1), :], (16, LANES)).astype(BF16)
            x.append(x_ref[row, h] * jnp.concatenate([mask] * (C // 16), axis=0))
        return dot(w_ref[0:4 * C, :], jnp.concatenate(x, axis=1))

    def ab_store(p, r, slot):
        for ab in range(2):
            for h in range(2):
                for c in range(0, C, WB):
                    at = 2 * (ab * C + c)
                    val, gate = p[at:at + WB, half(h)], p[at + WB:at + 2 * WB, half(h)]
                    s_ref[slot, h, pl.ds((ab * C + c) * ST + r, WB, stride=ST), :] = val * (jnp.tanh(gate) + 1.0)

    CB = CO // BG
    LBG = BG.bit_length() - 1

    def same(g):
        return g

    def ab_copy(k, group=same):
        c0 = pl.multiple_of((k & (BG - 1)) * CB, CB)
        rows = pl.ds(pl.multiple_of(mine + group(k >> LBG) * G, G), G)
        return pltpu.make_async_remote_copy(
            abs_ref.at[(k & (BG - 1))], ab_ref.at[:, pl.ds(c0, CB), :, rows, :],
            ab_send.at[(k & (BG - 1))], ab_recv.at[(k & (BG - 1))], device_id=partner, device_id_type=MESH)

    def spread_ab(k, group=same):
        g, c0 = (k >> LBG), (k & (BG - 1)) * CB
        own, other = (side * CO + c0) * ST, ((1 - side) * CO + c0) * ST
        s = s_ref.at[(g & 1)]
        here = ab_ref.at[:, pl.ds(c0, CB), :, pl.ds(pl.multiple_of(mine + group(g) * G, G), G), :]
        there = abs_ref.at[(k & (BG - 1))]
        for dc in range(CB):
            for ab in range(2):
                for h in range(2):
                    here[ab, dc, h] = s[h, pl.ds(own + (ab * C + dc) * ST, G), :].astype(BF16)
                    there[ab, dc, h] = s[h, pl.ds(other + (ab * C + dc) * ST, G), :].astype(BF16)

    def send_ab(k, group=same):
        @pl.when(k >= 0)
        def _():
            ab_copy(k, group).start()

        @pl.when(k + 1 >= BG)
        def _():
            ab_copy(k + 1 - BG, group).wait_send()

    def finish_ab(group=same):
        @pl.loop(NB - BG, NB)
        def _(k):
            spread_ab(k, group)
            send_ab(k, group)

    def drain_ab():
        for k in range(NB - BG + 1, NB):
            ab_copy(k).wait_send()

    EARLY = min(2, NG) * G

    def t_copy(c0, n, row0, rows, k):
        c0, rows = pl.multiple_of(c0, n), pl.ds(row0, rows)
        return pltpu.make_async_remote_copy(
            ts_ref.at[pl.ds(c0, n), :, rows, :], t_ref.at[pl.ds(side * CO + c0, n), :, rows, :],
            t_send.at[k], t_recv.at[k], device_id=partner, device_id_type=MESH)

    def early_t():
        return t_copy(0, CO, 0, EARLY, 0)

    def late_t(g):
        return t_copy(0, CO, pl.multiple_of(g * G, G), G, g)

    def recv_t(g):
        late_t(g).wait_recv()

    def triangle(outgoing, c):
        b = jnp.concatenate([ab_ref[1, c, 0], ab_ref[1, c, 1]], axis=1)
        if outgoing:
            a = jnp.concatenate([jnp.concatenate([ab_ref[0, c, h, pl.ds(r0, NR), :] for h in range(2)], axis=1)
                                 for r0 in (mine, theirs)], axis=0)
            t = dot(a, b, ((1,), (1,)))
        else:
            a = jnp.concatenate([ab_ref[0, c, side], ab_ref[0, c, 1 - side]], axis=1)
            t = dot(a, b, ((0,), (0,)))
        t = t.astype(BF16)
        for h in range(2):
            t_ref[side * CO + c, h] = t[:NR, half(h)]
            ts_ref[c, h] = t[NR:, half(h)]

    def triangles(outgoing):
        @pl.loop(0, TB)
        def _(cb):
            @pl.when(cb % (TB // BG) == 0 if BG < TB else cb >= 0)
            def _():
                for k in range(max(1, BG // TB)):
                    b = cb * BG // TB + k
                    arrived = ab_ref.at[:, pl.ds(b * CB, CB), :, pl.ds(theirs, NR), :]
                    pltpu.make_async_copy(arrived, arrived, ab_recv.at[b]).wait()
            for dc in range(CO // TB):
                triangle(outgoing, cb * (CO // TB) + dc)
            t_copy(cb * (CO // TB), CO // TB, 0, EARLY, 0).start()
        for g in range(EARLY // G, min(EARLY // G + 2, NG)):
            late_t(g).start()

    @pl.loop(0, NB + 1)
    def _(it):
        for pos in range(1, len(arrivals)):
            @pl.when(it == pos * BG)
            def _(pos=pos):
                arrived(pos)

        def row_of(step):
            return first_group(step >> LBG) * G + (step & (BG - 1)) * R

        k = it - 1 - BG
        row, now = row_of(jnp.maximum(it - 1, 0)), row_of(jnp.minimum(it, NB - 1))
        dots = [ab_dot(row + i) for i in range(R)]
        spread_ab(jnp.maximum(k, 0), first_group)
        for i in range(R):
            in_norm(now + i, [z_ref[now + i, 0], z_ref[now + i, 1]])
        prev = it - 1 + 2 * BG
        for i in range(R):
            ab_store(dots[i], (prev & (BG - 1)) * R + i, (prev >> LBG) & 1)
        send_ab(k, first_group)
    finish_ab(first_group)
    drain_gather()

    @pl.loop(0, n_upd)
    def _(u):
        prepare(u + 1)
        start(weight_copies(u + 2))

        @pl.when(u % 2 == 0)
        def _():
            triangles(True)

        @pl.when(u % 2 == 1)
        def _():
            triangles(False)

        drain_ab()
        early_t().wait_recv()

        @pl.when(u < n_upd - 1)
        def _():
            for c0 in range(0, C, 16):
                swap_t(0, c0, 16, 0)

            def norm_rows(it):
                for i in range(R):
                    y = out_norm((it & (BG - 1)) * R + i, (it >> LBG) & 1)
                    for h in range(2):
                        yb_ref[it & 1, i, h] = y[h]
                swap_t(jnp.minimum((it >> LBG) + 1, NG - 1), (it & (BG - 1)) * (C // BG), C // BG, ((it >> LBG) + 1) & 1)

            def store_rows(it, dots):
                prev = it - 2 + 2 * BG
                for i in range(R):
                    ab_store(dots[i], (prev & (BG - 1)) * R + i, (prev >> LBG) & 1)

            norm_rows(0)

            @pl.loop(1, NB + 1)
            def _(it):
                k = it - 2 - BG
                row1, row2 = (it - 1) * R, jnp.maximum(it - 2, 0) * R
                parts = {}
                for part, i in ORDER:
                    if part == "u":
                        parts["u", i] = upd_dot([yb_ref[(it + 1) & 1, i, h] for h in range(2)])
                    elif part == "g":
                        parts["g", i] = gate_dot(row1 + i)
                    else:
                        parts["a", i] = ab_dot(row2 + i)
                spread_ab(jnp.maximum(k, 0))
                norm_rows(it)
                for i in range(R):
                    in_norm(row1 + i, new_z(row1 + i, parts["u", i], parts["g", i]))
                store_rows(it, [parts["a", i] for i in range(R)])
                send_ab(k)

                g = ((it + 1) >> LBG) + 1

                @pl.when(jnp.logical_and(((it + 1) & (BG - 1)) == 0, g < NG - 2))
                def _():
                    late_t(g + 2).start()

                @pl.when(jnp.logical_and(((it + 1) & (BG - 1)) == 0, g < NG))
                def _():
                    recv_t(g)

            dots = [ab_dot((NB - 1) * R + i) for i in range(R)]
            spread_ab(NB - 1 - BG)
            store_rows(NB + 1, dots)
            send_ab(NB - 1 - BG)
            finish_ab()

        @pl.when(u == n_upd - 1)
        def _():
            for g in range(EARLY // G + 2, NG):
                late_t(g).start()
            for g in range(EARLY // G, NG):
                recv_t(g)
        early_t().wait_send()
        for g in range(EARLY // G, NG):
            late_t(g).wait_send()

    for cp in weight_copies(0):
        cp.wait()
    for c0 in range(0, C, 16):
        swap_t(q, c0, 16, 0)

    @pl.loop(0, G, step=4)
    def _(r0):
        outs = [(upd_dot(out_norm(r0 + i, 0)), gate_dot(q * G + r0 + i)) for i in range(4)]
        for i in range(4):
            z_row = new_z(q * G + r0 + i, *outs[i])
            for h in range(2):
                z_t = z_row[h].T
                for k, (a, b) in enumerate(pieces(h)):
                    ts_ref[r0 + i, a, b:b + G, :] = z_t[k * G:(k + 1) * G]
    cp = pltpu.make_async_copy(ts_ref.at[pl.ds(0, G)], out, in_sem.at[0])
    cp.start()
    cp.wait()


def solution(mesh):
    nz, ny = mesh.shape["dap2"], mesh.shape["dap"] // 2
    row_spec = P(ALL_ROWS, None, None)
    mask_spec = P(ALL_ROWS, None)

    def local_stack(pair_rep, pair_mask, norm_in, norm_out, w_ab, w_gate, w_out):
        G, N = pair_rep.shape[:2]
        NR, n_upd = N // 2, 2 * w_ab.shape[0]
        norms = jnp.concatenate([norm_in.reshape(-1, C), norm_out.reshape(-1, C)]).astype(F32)
        BG = G // R
        anyspec = pl.BlockSpec(memory_space=pl.ANY)
        vmem = pl.BlockSpec(memory_space=pltpu.VMEM)
        dma = pltpu.SemaphoreType.DMA
        n_gather = 2 * (nz - 1) + nz
        o = pl.pallas_call(
            functools.partial(kernel, nz, ny, n_upd),
            out_shape=jax.ShapeDtypeStruct((G, 2, NR, C), BF16),
            in_specs=[anyspec, anyspec, vmem, anyspec, anyspec, anyspec],
            out_specs=anyspec,
            scratch_shapes=[
                pltpu.VMEM((NR, 2, C, LANES), BF16),
                pltpu.VMEM((NR, 2, C, LANES), BF16),
                pltpu.VMEM((2, CO, 2, N, LANES), BF16),
                pltpu.VMEM((C, 2, NR, LANES), BF16),
                pltpu.VMEM((CO, 2, NR, LANES), BF16),
                pltpu.VMEM((BG, 2, CO // BG, 2, G, LANES), BF16),
                pltpu.VMEM((2, 2, 2 * C * (G + 1), LANES), F32),
                pltpu.VMEM((2, 2, G * Y_PITCH, LANES), F32),
                pltpu.VMEM((2, R, 2, C, LANES), BF16),
                pltpu.VMEM((2, NR, LANES), F32),
                pltpu.VMEM((G, N), jnp.int32),
                pltpu.VMEM((C, 6 * C), BF16),
                pltpu.VMEM((6 * C, C), BF16),
                pltpu.VMEM((4, C, LANES), F32),
                dma((2,)), dma((3,)),
                dma((n_gather,)), dma((n_gather,)), dma((n_gather,)), dma((n_gather,)),
                dma((BG,)), dma((BG,)), dma((NR // G,)), dma((NR // G,)),
            ],
            compiler_params=pltpu.CompilerParams(collective_id=0, has_side_effects=True, vmem_limit_bytes=67043328),
        )(pair_rep.reshape(G, 2, NR, C), pair_mask, norms, w_ab.reshape(n_upd, C, 4 * C), w_gate.reshape(n_upd, C, C), w_out.reshape(n_upd, C, C))
        return o.reshape(G, N, C)

    return jax.shard_map(local_stack, mesh=mesh, in_specs=(row_spec, mask_spec, P(), P(), P(), P(), P()), out_specs=row_spec, check_vma=False)
```
